32 devices in a mesh: lat: 16 (over z, x, core), lon: 2 (over y).
Axes of the slice: x: 2, y: 2, z: 4, core: 2. Of those that a mesh axis runs over, the one named last changes fastest.
Arguments:
- elevation: float32 [4096, 4096], P('lat', 'lon'), may hold values from -200 to 200
Outputs:
- slope_angle: float32 [4096, 4096], P('lat', 'lon')
- facing: float32 [2, 4096, 4096], P(None, 'lat', 'lon')
- hillshade: float32 [4096, 4096], P('lat', 'lon')
The draws below stay inside these ranges and needn't reach their ends.
All inputs are finite; a program needn't handle non-finite values.
Results may differ from the reference program's by a relative error of at most 0.0003.
Values sent between devices are 32-bit elements; how exact they have to be, the bound alone decides.
No kernel may reach another device: no remote copies, remote signals or barrier semaphores. Data moves between devices by JAX's collectives and lax.ppermute only.
A program may use at most 64 MiB of HBM per device.

```python
import math
import jax
import jax.numpy as jnp
from jax import lax

SCALES = 7
HALO = 64
NROWS = 4096
NCOLS = 4096


def draw_elevation(key, part):
    surface = jnp.zeros((NROWS, NCOLS), jnp.float32)
    for octave in range(SCALES):
        stride = 2 ** octave
        noise_key = jax.random.fold_in(key, 11 + octave)
        shift_key = jax.random.fold_in(key, 101 + octave)
        coarse_shape = (NROWS // stride, NCOLS // stride)
        coarse = jax.random.truncated_normal(noise_key, -4.0, 4.0, coarse_shape, jnp.float32)
        amplitude = 2.0 * math.sqrt(stride)
        upsampled = jnp.repeat(jnp.repeat(coarse, stride, axis=0), stride, axis=1)
        offsets = jax.random.randint(shift_key, (2,), 0, stride)
        upsampled = jnp.roll(upsampled, (offsets[0], offsets[1]), axis=(0, 1))
        surface = surface + amplitude * upsampled
    return surface


def setup_inputs(seed: int = 0) -> dict:
    streams_of = jax.random.split(jax.random.key(seed), 2)
    elevation = draw_elevation(jax.random.fold_in(streams_of[1], 71), 0)
    return dict(elevation=elevation)


LIGHT_EAST = -0.5
LIGHT_NORTH = 0.5
LIGHT_UP = math.sqrt(0.5)

def window(padded, margin, row_offset, col_offset, row_count, col_count):
    return lax.slice(padded, (margin + row_offset, margin + col_offset), (margin + row_offset + row_count, margin + col_offset + col_count))

def terrain_shading(padded, spacing, margin, levels):
    row_count = padded.shape[0] - 2 * margin
    col_count = padded.shape[1] - 2 * margin
    eastward = jnp.zeros((row_count, col_count), jnp.float32)
    northward = jnp.zeros((row_count, col_count), jnp.float32)
    for octave in range(levels):
        stride = 2 ** octave
        north_west = window(padded, margin, -stride, -stride, row_count, col_count)
        north_mid = window(padded, margin, -stride, 0, row_count, col_count)
        north_east = window(padded, margin, -stride, stride, row_count, col_count)
        west_mid = window(padded, margin, 0, -stride, row_count, col_count)
        east_mid = window(padded, margin, 0, stride, row_count, col_count)
        south_west = window(padded, margin, stride, -stride, row_count, col_count)
        south_mid = window(padded, margin, stride, 0, row_count, col_count)
        south_east = window(padded, margin, stride, stride, row_count, col_count)
        east_diff = north_east + 2.0 * east_mid + south_east - (north_west + 2.0 * west_mid + south_west)
        north_diff = north_west + 2.0 * north_mid + north_east - (south_west + 2.0 * south_mid + south_east)
        eastward = eastward + east_diff * (1.0 / stride)
        northward = northward + north_diff * (1.0 / stride)
    grad_east = eastward / (8.0 * levels * spacing[:, None])
    grad_north = northward * (1.0 / (8.0 * levels))
    squared = grad_east * grad_east + grad_north * grad_north
    slope_angle = jnp.arctan(jnp.sqrt(squared))
    inverse = lax.rsqrt(1.0 + squared)
    facing_east = -grad_east * inverse
    facing_north = -grad_north * inverse
    shading = jnp.maximum(LIGHT_EAST * facing_east + LIGHT_NORTH * facing_north + LIGHT_UP * inverse, 0.0)
    return (slope_angle, jnp.stack([facing_east, facing_north]), shading)

def reference(elevation):
    margin = HALO
    wrapped = jnp.concatenate([elevation[:, NCOLS - margin:], elevation, elevation[:, :margin]], axis=1)
    padded = jnp.concatenate([jnp.broadcast_to(wrapped[:1], (margin, NCOLS + 2 * margin)), wrapped, jnp.broadcast_to(wrapped[NROWS - 1:], (margin, NCOLS + 2 * margin))], axis=0)
    position = jnp.arange(NROWS, dtype=jnp.int32)
    spacing = jnp.sin((position.astype(jnp.float32) + 0.5) * (math.pi / NROWS)) * (2.0 * NROWS / NCOLS)
    block_rows = math.gcd(NROWS, 512)
    block_count = NROWS // block_rows

    def one_block(number):
        first_row = (number * block_rows).astype(jnp.int32)
        slab = lax.dynamic_slice(padded, (first_row, jnp.int32(0)), (block_rows + 2 * margin, NCOLS + 2 * margin))
        slab_spacing = lax.dynamic_slice(spacing, (first_row,), (block_rows,))
        return terrain_shading(slab, slab_spacing, margin, SCALES)
    results = lax.map(one_block, jnp.arange(block_count, dtype=jnp.int32))
    slope_angle = results[0].reshape(NROWS, NCOLS)
    facing = jnp.transpose(results[1], (1, 0, 2, 3)).reshape(2, NROWS, NCOLS)
    hillshade = results[2].reshape(NROWS, NCOLS)
    return (slope_angle, facing, hillshade)
```

```python
import functools
import math

import jax
import jax.numpy as jnp
from jax import lax
from jax.experimental import pallas as pl
from jax.experimental.pallas import tpu as pltpu
from jax.sharding import PartitionSpec as P

SCALES = 7
HALO = 64
LANES = 128
SUB = 8

LIGHT_UP = math.sqrt(0.5)
TINY = 1.17549435e-38

ACOS_FIT = (
    0.036142768221257435,
    -0.1987486877325598,
    0.5130441168137142,
    -0.9077345836840529,
    1.5572964573334291,
)
ANGLE_FIT = tuple(
    c * math.sqrt(2.0) * math.sqrt(0.5) ** (len(ACOS_FIT) - 1 - i) for i, c in enumerate(ACOS_FIT)
)


def shade(east, north, east_scale):
    neg_east = east * east_scale
    neg_north = north * (-1.0 / (8.0 * SCALES))
    squared = neg_east * neg_east + neg_north * neg_north
    inverse = lax.rsqrt(1.0 + squared)
    facing_east = neg_east * inverse
    facing_north = neg_north * inverse
    shading = jnp.maximum(inverse * (0.5 * (neg_north - neg_east) + LIGHT_UP), 0.0)
    sine = squared * lax.rsqrt(jnp.maximum(squared, TINY)) * inverse
    cos_one = 1.0 + inverse
    root = lax.rsqrt(cos_one)
    half = cos_one * root
    fit = ANGLE_FIT[0]
    for coefficient in ANGLE_FIT[1:]:
        fit = fit * half + coefficient
    slope = sine * root * fit
    return slope, facing_east, facing_north, shading


def stencil(z, q, scale, out, row_count, tiles):
    lane = lax.broadcasted_iota(jnp.int32, (SUB, LANES), 1)
    lags = [2**k for k in range(SCALES)]

    def steps(lag):
        return -(-lag // SUB)

    def new_boxes(base, active, tile_cache):
        here = [z[j, pl.ds(base + HALO, SUB), :] for j in range(tiles + 1)]
        for k in active:
            s = lags[k]
            pairs = []
            for j in range(tiles + 1):
                pair = z[j, pl.ds(base + HALO + s, SUB), :] + here[j]
                pairs.append(pair * (1.0 / s) if k else pair)
            if 2 * s == LANES:
                halves = [
                    pltpu.roll(jnp.where(lane >= s, pairs[j], pairs[(j + 1) % (tiles + 1)]), s, 1)
                    for j in range(tiles + 1)
                ]
            for j in range(tiles):
                before, after = pairs[(j - 1) % (tiles + 1)], pairs[j + 1]
                if 2 * s == LANES:
                    west, east = halves[(j - 1) % (tiles + 1)], halves[j]
                else:
                    west = pltpu.roll(jnp.where(lane < LANES - s, pairs[j], before), s, 1)
                    east = pltpu.roll(jnp.where(lane >= s, pairs[j], after), LANES - s, 1)
                low, high = pairs[j] + west, pairs[j] + east
                old = tile_cache.get("old") is not None
                if s < SUB:
                    q[k][0, j, pl.ds(base + s + SUB, SUB), :] = low
                    q[k][1, j, pl.ds(base + s + SUB, SUB), :] = high
                    if old:
                        before = q[k][0, j, pl.ds(base + SUB, SUB), :]
                        after = q[k][1, j, pl.ds(base + SUB, SUB), :]
                else:
                    slot = lax.bitwise_and(base // SUB, s // SUB - 1)
                    row = pl.multiple_of(slot * SUB, SUB)
                    if old:
                        before = q[k][0, j, pl.ds(row, SUB), :]
                        after = q[k][1, j, pl.ds(row, SUB), :]
                    q[k][0, j, pl.ds(row, SUB), :] = low
                    q[k][1, j, pl.ds(row, SUB), :] = high
                if old:
                    tile_cache[j, k] = (low, high, before, after)

    def warm(step, active):
        new_boxes(step * SUB, active, {})

    edges = sorted({-steps(s) for s in lags}) + [0]
    for first, last in zip(edges[:-1], edges[1:]):
        active = [k for k, s in enumerate(lags) if -steps(s) <= first]

        @pl.loop(first, last)
        def _(step, active=active):
            warm(step, active)

    @pl.loop(0, row_count // SUB)
    def _(step):
        base = pl.multiple_of(step * SUB, SUB)
        cache = {"old": True}
        new_boxes(base, range(SCALES), cache)
        east_scale = scale[pl.ds(base, SUB), :]
        for j in range(tiles):
            falling = rising = None
            for k in range(SCALES):
                low, high, old_low, old_high = cache[j, k]
                down, up = old_high - low, high - old_low
                falling = down if falling is None else falling + down
                rising = up if rising is None else rising + up
            results = shade(falling + rising, falling - rising, east_scale)
            for n, value in enumerate(results):
                out[n, pl.ds(base, SUB), j * LANES : (j + 1) * LANES] = value


def load_columns(source, row0, rows, z, z_row0, first, count, sem):
    copies = []
    for j in range(count):
        copies.append(
            pltpu.make_async_copy(
                source.at[pl.ds(row0, rows), j * LANES : (j + 1) * LANES],
                z.at[first + j, pl.ds(z_row0, rows), :],
                sem.at[first + j],
            )
        )
    return copies


def store_rows(out, slope, facing, shading, row0, rows, sem):
    targets = (slope, facing.at[0], facing.at[1], shading)
    return [
        pltpu.make_async_copy(out.at[n], target.at[pl.ds(row0, rows), :], sem.at[n])
        for n, target in enumerate(targets)
    ]


def main_kernel(rows, tiles, where, x, lon, near, scale, slope, facing, shading, *scratch):
    z, out, scale_v, sem_x, sem_near, sem_scale, sem_out = scratch[:7]
    q = scratch[7:]
    odd = where[0]
    own = pl.multiple_of(odd * HALO, HALO)
    beyond = pl.multiple_of((1 - odd) * rows, HALO)
    row0 = pl.multiple_of((1 - odd) * HALO, HALO)
    copies = load_columns(x, 0, rows, z, own, 0, tiles, sem_x)
    copies += load_columns(lon, 0, rows, z, own, tiles, 1, sem_x)
    copies += load_columns(near, 0, HALO, z, beyond, 0, tiles + 1, sem_near)
    copies.append(pltpu.make_async_copy(scale.at[pl.ds(row0, rows - HALO), :], scale_v, sem_scale))
    for copy in copies:
        copy.start()
    for copy in copies:
        copy.wait()
    stencil(z, q, scale_v, out, rows - HALO, tiles)
    stores = store_rows(out, slope, facing, shading, row0, rows - HALO, sem_out)
    for copy in stores:
        copy.start()
    for copy in stores:
        copy.wait()


def rim_kernel(
    rows, tiles, where, x, lon, far, far_lon, scale, _a, _b, _c, slope, facing, shading, *scratch
):
    z, out, scale_v, sem_x, sem_far, sem_scale, sem_out = scratch[:7]
    q = scratch[7:]
    odd, pole = where[0], where[1]
    span = 2 * HALO
    own = pl.multiple_of((1 - odd) * HALO, HALO)
    beyond = pl.multiple_of(odd * span, HALO)
    first = pl.multiple_of(odd * (rows - span), HALO)
    row0 = pl.multiple_of(odd * (rows - HALO), HALO)
    copies = load_columns(x, first, span, z, own, 0, tiles, sem_x)
    copies += load_columns(lon, first, span, z, own, tiles, 1, sem_x)
    copies += load_columns(far, 0, HALO, z, beyond, 0, tiles, sem_far)
    copies += load_columns(far_lon, 0, HALO, z, beyond, tiles, 1, sem_far)
    copies.append(pltpu.make_async_copy(scale.at[pl.ds(row0, HALO), :], scale_v, sem_scale))
    for copy in copies:
        copy.start()
    for copy in copies:
        copy.wait()

    @pl.when(jnp.logical_and(pole == 1, odd == 0))
    def _():
        for j in range(tiles + 1):
            z[j, 0:HALO, :] = jnp.broadcast_to(z[j, HALO : HALO + 1, :], (HALO, LANES))

    @pl.when(jnp.logical_and(pole == 1, odd == 1))
    def _():
        for j in range(tiles + 1):
            z[j, span:, :] = jnp.broadcast_to(z[j, span - 1 : span, :], (HALO, LANES))

    stencil(z, q, scale_v, out, HALO, tiles)
    stores = store_rows(out, slope, facing, shading, row0, HALO, sem_out)
    for copy in stores:
        copy.start()
    for copy in stores:
        copy.wait()


def scratch_for(out_rows, tiles):
    return [
        pltpu.VMEM((tiles + 1, out_rows + 2 * HALO, LANES), jnp.float32),
        pltpu.VMEM((4, out_rows, tiles * LANES), jnp.float32),
        pltpu.VMEM((out_rows, LANES), jnp.float32),
        pltpu.SemaphoreType.DMA((tiles + 1,)),
        pltpu.SemaphoreType.DMA((tiles + 1,)),
        pltpu.SemaphoreType.DMA,
        pltpu.SemaphoreType.DMA((4,)),
    ] + [
        pltpu.VMEM((2, tiles, out_rows + 3 * SUB if 2**k < SUB else 2**k, LANES), jnp.float32)
        for k in range(SCALES)
    ]


def cost(out_rows, cols):
    cells = out_rows * cols
    return pl.CostEstimate(flops=200 * cells, bytes_accessed=24 * cells, transcendentals=3 * cells)


def lon_halo(x):
    count = lax.axis_size("lon")
    first, last = x[:, :HALO], x[:, x.shape[1] - HALO :]
    if count == 2:
        both = jnp.concatenate([first, last], axis=1)
        return lax.ppermute(both, "lon", [(0, 1), (1, 0)])
    westward = [(i, (i - 1) % count) for i in range(count)]
    eastward = [(i, (i + 1) % count) for i in range(count)]
    return jnp.concatenate(
        [lax.ppermute(first, "lon", westward), lax.ppermute(last, "lon", eastward)], axis=1
    )


def pairs(first, count):
    ends = [(i, i + 1) for i in range(first, count - 1, 2)]
    return ends + [(b, a) for a, b in ends]


def local(x):
    rows, cols = x.shape
    tiles = cols // LANES
    lat = lax.axis_index("lat")
    count = lax.axis_size("lat")
    odd = lat % 2
    far_row = odd * (rows - HALO)
    near_row = (1 - odd) * (rows - HALO)

    far = lax.ppermute(lax.dynamic_slice(x, (far_row, 0), (HALO, cols)), "lat", pairs(1, count))
    lon = lon_halo(x)
    near_block = jnp.concatenate(
        [
            lax.dynamic_slice(x, (near_row, 0), (HALO, cols)),
            lax.dynamic_slice(lon, (near_row, 0), (HALO, LANES)),
        ],
        axis=1,
    )
    near = lax.ppermute(near_block, "lat", pairs(0, count))
    far_lon = lax.ppermute(
        lax.dynamic_slice(lon, (far_row, 0), (HALO, LANES)), "lat", pairs(1, count)
    )

    total_rows = rows * count
    total_cols = cols * lax.axis_size("lon")
    position = lat * rows + lax.broadcasted_iota(jnp.int32, (rows, LANES), 0)
    spacing = jnp.sin((position.astype(jnp.float32) + 0.5) * (math.pi / total_rows)) * (
        2.0 * total_rows / total_cols
    )
    scale = -1.0 / (8.0 * SCALES * spacing)
    pole = jnp.logical_or(lat == 0, lat == count - 1)
    where = jnp.stack([odd.astype(jnp.int32), pole.astype(jnp.int32)])

    shapes = [
        jax.ShapeDtypeStruct((rows, cols), jnp.float32),
        jax.ShapeDtypeStruct((2, rows, cols), jnp.float32),
        jax.ShapeDtypeStruct((rows, cols), jnp.float32),
    ]
    smem = pl.BlockSpec(memory_space=pltpu.SMEM)
    anywhere = pl.BlockSpec(memory_space=pl.ANY)
    hbm = pl.BlockSpec(memory_space=pltpu.HBM)
    outs = pl.pallas_call(
        functools.partial(main_kernel, rows, tiles),
        out_shape=shapes,
        in_specs=[smem] + [anywhere] * 4,
        out_specs=[hbm] * 3,
        scratch_shapes=scratch_for(rows - HALO, tiles),
        cost_estimate=cost(rows - HALO, cols),
        compiler_params=pltpu.CompilerParams(vmem_limit_bytes=58 * 2**20),
        name="stencil_main",
    )(where, x, lon, near, scale)
    return tuple(
        pl.pallas_call(
            functools.partial(rim_kernel, rows, tiles),
            out_shape=shapes,
            in_specs=[smem] + [anywhere] * 5 + [hbm] * 3,
            out_specs=[hbm] * 3,
            input_output_aliases={6: 0, 7: 1, 8: 2},
            scratch_shapes=scratch_for(HALO, tiles),
            cost_estimate=cost(HALO, cols),
            compiler_params=pltpu.CompilerParams(vmem_limit_bytes=40 * 2**20),
            name="stencil_rim",
        )(where, x, lon, far, far_lon, scale, *outs)
    )


def solution(mesh):
    in_specs = (P("lat", "lon"),)
    out_specs = (P("lat", "lon"), P(None, "lat", "lon"), P("lat", "lon"))
    return jax.shard_map(local, mesh=mesh, in_specs=in_specs, out_specs=out_specs, check_vma=False)
```

```python
import functools
import math

import jax
import jax.numpy as jnp
from jax import lax
from jax.experimental import pallas as pl
from jax.experimental.pallas import tpu as pltpu
from jax.sharding import PartitionSpec as P


SCALES = 7
HALO = 64
LANES = 128
SUB = 8
VMEM_LIMIT = 48 * 2**20
HALO_SPACE = pltpu.VMEM

LIGHT_UP = math.sqrt(0.5)
TINY = 1.17549435e-38

SINE_FIT = tuple((-1.0) ** k / math.factorial(2 * k + 1) for k in range(7, -1, -1))
ACOS_FIT = (
    0.036142768221257435,
    -0.1987486877325598,
    0.5130441168137142,
    -0.9077345836840529,
    1.5572964573334291,
)
ANGLE_FIT = tuple(
    c * math.sqrt(2.0) * math.sqrt(0.5) ** (len(ACOS_FIT) - 1 - i) for i, c in enumerate(ACOS_FIT)
)


def shade(east, north, east_scale):
    neg_east = east * east_scale
    neg_north = north * (-1.0 / (8.0 * SCALES))
    squared = neg_east * neg_east + neg_north * neg_north
    inverse = lax.rsqrt(1.0 + squared)
    facing_east = neg_east * inverse
    facing_north = neg_north * inverse
    shading = jnp.maximum(inverse * (0.5 * (neg_north - neg_east) + LIGHT_UP), 0.0)
    sine = squared * lax.rsqrt(jnp.maximum(squared, TINY)) * inverse
    cos_one = 1.0 + inverse
    root = lax.rsqrt(cos_one)
    half = cos_one * root
    fit = ANGLE_FIT[0]
    for coefficient in ANGLE_FIT[1:]:
        fit = fit * half + coefficient
    slope = sine * root * fit
    return slope, facing_east, facing_north, shading


def row_scale(row0, total_rows, total_cols):
    row = row0 + lax.broadcasted_iota(jnp.int32, (SUB, LANES), 0)
    turn = (row.astype(jnp.float32) + 0.5) * (1.0 / total_rows)
    angle = jnp.minimum(turn, 1.0 - turn) * math.pi
    power = angle * angle
    sine = jnp.full_like(angle, SINE_FIT[0])
    for coefficient in SINE_FIT[1:]:
        sine = sine * power + coefficient
    spacing = angle * sine * (2.0 * total_rows / total_cols)
    return -1.0 / (8.0 * SCALES * spacing)


def stencil(z, q, first_row, total, out, held, store, row_count, tiles):
    lane = lax.broadcasted_iota(jnp.int32, (SUB, LANES), 1)
    lags = [2**k for k in range(SCALES)]

    def steps(lag):
        return -(-lag // SUB)

    def new_boxes(base, active, tile_cache):
        here = [z[j, pl.ds(base + HALO, SUB), :] for j in range(tiles + 1)]
        for k in active:
            s = lags[k]
            pairs = []
            for j in range(tiles + 1):
                pair = z[j, pl.ds(base + HALO + s, SUB), :] + here[j]
                pairs.append(pair * (1.0 / s) if k else pair)
            if 2 * s == LANES:
                halves = [
                    pltpu.roll(jnp.where(lane >= s, pairs[j], pairs[(j + 1) % (tiles + 1)]), s, 1)
                    for j in range(tiles + 1)
                ]
            for j in range(tiles):
                before, after = pairs[(j - 1) % (tiles + 1)], pairs[j + 1]
                if 2 * s == LANES:
                    west, east = halves[(j - 1) % (tiles + 1)], halves[j]
                else:
                    west = pltpu.roll(jnp.where(lane < LANES - s, pairs[j], before), s, 1)
                    east = pltpu.roll(jnp.where(lane >= s, pairs[j], after), LANES - s, 1)
                low, high = pairs[j] + west, pairs[j] + east
                old = tile_cache.get("old") is not None
                if s < SUB:
                    q[k][0, j, pl.ds(base + s + SUB, SUB), :] = low
                    q[k][1, j, pl.ds(base + s + SUB, SUB), :] = high
                    if old:
                        before = q[k][0, j, pl.ds(base + SUB, SUB), :]
                        after = q[k][1, j, pl.ds(base + SUB, SUB), :]
                else:
                    slot = lax.bitwise_and(base // SUB, s // SUB - 1)
                    row = pl.multiple_of(slot * SUB, SUB)
                    if old:
                        before = q[k][0, j, pl.ds(row, SUB), :]
                        after = q[k][1, j, pl.ds(row, SUB), :]
                    q[k][0, j, pl.ds(row, SUB), :] = low
                    q[k][1, j, pl.ds(row, SUB), :] = high
                if old:
                    tile_cache[j, k] = (low, high, before, after)

    def warm(step, active):
        new_boxes(step * SUB, active, {})

    edges = sorted({-steps(s) for s in lags}) + [0]
    for first, last in zip(edges[:-1], edges[1:]):
        active = [k for k, s in enumerate(lags) if -steps(s) <= first]

        @pl.loop(first, last)
        def _(step, active=active):
            warm(step, active)

    def sums(step):
        base = pl.multiple_of(step * SUB, SUB)
        cache = {"old": True}
        new_boxes(base, range(SCALES), cache)
        for j in range(tiles):
            falling = rising = None
            for k in range(SCALES):
                low, high, old_low, old_high = cache[j, k]
                down, up = old_high - low, high - old_low
                falling = down if falling is None else falling + down
                rising = up if rising is None else rising + up
            held[0, j] = falling + rising
            held[1, j] = falling - rising

    def finish(step):
        base = pl.multiple_of(step * SUB, SUB)
        east_scale = row_scale(first_row + base, *total)
        for j in range(tiles):
            results = shade(held[0, j], held[1, j], east_scale)
            for n, value in enumerate(results):
                out[n, pl.ds(base, SUB), j * LANES : (j + 1) * LANES] = value

    count = row_count // SUB

    @pl.loop(0, count)
    def _(step):
        finish(jnp.maximum(step - 1, 0))
        sums(step)

        @pl.when(step > 0)
        def _():
            for copy in store(step - 1):
                copy.start()

    finish(count - 1)
    for copy in store(count - 1):
        copy.start()


def column_copies(source, row0, rows, z, z_row0, first, count, sem):
    return [
        pltpu.make_async_copy(
            source.at[pl.ds(row0, rows), j * LANES : (j + 1) * LANES],
            z.at[first + j, pl.ds(z_row0, rows), :],
            sem.at[first + j],
        )
        for j in range(count)
    ]


def row_copies(out, targets, out_row, row0, rows, sem):
    slope, facing, shading = targets
    places = (slope, facing.at[0], facing.at[1], shading)
    return [
        pltpu.make_async_copy(
            out.at[n, pl.ds(out_row, rows), :], place.at[pl.ds(row0, rows), :], sem.at[n]
        )
        for n, place in enumerate(places)
    ]


def run(copies):
    for copy in copies:
        copy.start()
    for copy in copies:
        copy.wait()


def write_rows(z, q, held, out, sem, targets, row0, lat, total, rows, out_rows, tiles):
    def store(step):
        base = pl.multiple_of(step * SUB, SUB)
        return row_copies(out, targets, base, pl.multiple_of(row0 + base, SUB), SUB, sem)

    stencil(z, q, lat * rows + row0, total, out, held, store, out_rows, tiles)
    for copy in row_copies(out, targets, 0, row0, out_rows, sem):
        copy.wait()


def main_kernel(rows, tiles, total, x, lon, near, slope, facing, shading, *scratch):
    z, out, held, sem_x, sem_near, sem_out = scratch[:6]
    lat = lax.axis_index("lat")
    odd = lax.rem(lat, 2)
    own = pl.multiple_of(odd * HALO, HALO)
    beyond = pl.multiple_of((1 - odd) * rows, HALO)
    row0 = pl.multiple_of((1 - odd) * HALO, HALO)
    run(
        column_copies(x, 0, rows, z, own, 0, tiles, sem_x)
        + column_copies(lon, 0, rows, z, own, tiles, 1, sem_x)
        + column_copies(near, 0, HALO, z, beyond, 0, tiles + 1, sem_near)
    )
    write_rows(
        z, scratch[6:], held, out, sem_out, (slope, facing, shading), row0, lat, total, rows,
        rows - HALO, tiles,
    )


def rim_kernel(
    rows, tiles, total, lat_count, x, lon, far, far_lon, _a, _b, _c, slope, facing, shading, *scratch
):
    z, out, held, sem_x, sem_far, sem_out = scratch[:6]
    lat = lax.axis_index("lat")
    odd = lax.rem(lat, 2)
    span = 2 * HALO
    own = pl.multiple_of((1 - odd) * HALO, HALO)
    beyond = pl.multiple_of(odd * span, HALO)
    first = pl.multiple_of(odd * (rows - span), HALO)
    row0 = pl.multiple_of(odd * (rows - HALO), HALO)
    run(
        column_copies(x, first, span, z, own, 0, tiles, sem_x)
        + column_copies(lon, first, span, z, own, tiles, 1, sem_x)
        + column_copies(far, 0, HALO, z, beyond, 0, tiles, sem_far)
        + column_copies(far_lon, 0, HALO, z, beyond, tiles, 1, sem_far)
    )

    @pl.when(lat == 0)
    def _():
        for j in range(tiles + 1):
            z[j, 0:HALO, :] = jnp.broadcast_to(z[j, HALO : HALO + 1, :], (HALO, LANES))

    @pl.when(lat == lat_count - 1)
    def _():
        for j in range(tiles + 1):
            z[j, span:, :] = jnp.broadcast_to(z[j, span - 1 : span, :], (HALO, LANES))

    write_rows(
        z, scratch[6:], held, out, sem_out, (slope, facing, shading), row0, lat, total, rows,
        HALO, tiles,
    )


def scratch_for(out_rows, tiles):
    return [
        pltpu.VMEM((tiles + 1, out_rows + 2 * HALO, LANES), jnp.float32),
        pltpu.VMEM((4, out_rows, tiles * LANES), jnp.float32),
        pltpu.VMEM((2, tiles, SUB, LANES), jnp.float32),
        pltpu.SemaphoreType.DMA((tiles + 1,)),
        pltpu.SemaphoreType.DMA((tiles + 1,)),
        pltpu.SemaphoreType.DMA((4,)),
    ] + [
        pltpu.VMEM((2, tiles, out_rows + 3 * SUB if 2**k < SUB else 2**k, LANES), jnp.float32)
        for k in range(SCALES)
    ]


def cost(out_rows, cols):
    cells = out_rows * cols
    return pl.CostEstimate(flops=200 * cells, bytes_accessed=24 * cells, transcendentals=3 * cells)


def lon_halo(x):
    count = lax.axis_size("lon")
    cols = x.shape[1]
    if count == 2:
        lane = lax.broadcasted_iota(jnp.int32, (x.shape[0], LANES), 1)
        both = jnp.where(lane < HALO, x[:, :LANES], x[:, cols - LANES :])
        return lax.ppermute(both, "lon", [(0, 1), (1, 0)])
    westward = [(i, (i - 1) % count) for i in range(count)]
    eastward = [(i, (i + 1) % count) for i in range(count)]
    east = lax.ppermute(x[:, :HALO], "lon", westward)
    west = lax.ppermute(x[:, cols - HALO :], "lon", eastward)
    return jnp.concatenate([east, west], axis=1)


def pairs(first, count):
    ends = [(i, i + 1) for i in range(first, count - 1, 2)]
    return ends + [(b, a) for a, b in ends]


def local(x):
    rows, cols = x.shape
    tiles = cols // LANES
    lat = lax.axis_index("lat")
    count = lax.axis_size("lat")
    odd = lax.rem(lat, 2)
    far_row = odd * (rows - HALO)
    near_row = (1 - odd) * (rows - HALO)

    far_block = lax.dynamic_slice(x, (far_row, 0), (HALO, cols))
    far = lax.ppermute(far_block, "lat", pairs(1, count))
    lon = lon_halo(x)
    near_block = jnp.concatenate(
        [
            lax.dynamic_slice(x, (near_row, 0), (HALO, cols)),
            lax.dynamic_slice(lon, (near_row, 0), (HALO, LANES)),
        ],
        axis=1,
    )
    near = lax.ppermute(near_block, "lat", pairs(0, count))
    corner_block = lax.dynamic_slice(lon, (far_row, 0), (HALO, LANES))
    far_lon = lax.ppermute(corner_block, "lat", pairs(1, count))

    total = (rows * count, cols * lax.axis_size("lon"))
    shapes = [
        jax.ShapeDtypeStruct((rows, cols), jnp.float32),
        jax.ShapeDtypeStruct((2, rows, cols), jnp.float32),
        jax.ShapeDtypeStruct((rows, cols), jnp.float32),
    ]
    hbm = pl.BlockSpec(memory_space=pltpu.HBM)
    halo = pl.BlockSpec(memory_space=HALO_SPACE)
    outs = pl.pallas_call(
        functools.partial(main_kernel, rows, tiles, total),
        out_shape=shapes,
        in_specs=[hbm, halo, halo],
        out_specs=[hbm] * 3,
        scratch_shapes=scratch_for(rows - HALO, tiles),
        cost_estimate=cost(rows - HALO, cols),
        compiler_params=pltpu.CompilerParams(vmem_limit_bytes=VMEM_LIMIT),
        name="stencil_main",
    )(x, lon, near)
    return tuple(
        pl.pallas_call(
            functools.partial(rim_kernel, rows, tiles, total, count),
            out_shape=shapes,
            in_specs=[hbm] + [halo] * 3 + [hbm] * 3,
            out_specs=[hbm] * 3,
            input_output_aliases={4: 0, 5: 1, 6: 2},
            scratch_shapes=scratch_for(HALO, tiles),
            cost_estimate=cost(HALO, cols),
            compiler_params=pltpu.CompilerParams(vmem_limit_bytes=VMEM_LIMIT),
            name="stencil_rim",
        )(x, lon, far, far_lon, *outs)
    )


def solution(mesh):
    in_specs = (P("lat", "lon"),)
    out_specs = (P("lat", "lon"), P(None, "lat", "lon"), P("lat", "lon"))

    return jax.shard_map(local, mesh=mesh, in_specs=in_specs, out_specs=out_specs, check_vma=False)
```

```python
import functools
import math

import jax
import jax.numpy as jnp
from jax import lax
from jax.experimental import pallas as pl
from jax.experimental.pallas import tpu as pltpu
from jax.sharding import PartitionSpec as P


SCALES = 7
HALO = 64
LANES = 128
SUB = 8
VMEM_LIMIT = 48 * 2**20
HALO_SPACE = pltpu.VMEM

LIGHT_UP = math.sqrt(0.5)
TINY = 1.17549435e-38

SINE_FIT = tuple((-1.0) ** k / math.factorial(2 * k + 1) for k in range(7, -1, -1))
ACOS_FIT = (
    0.036142768221257435,
    -0.1987486877325598,
    0.5130441168137142,
    -0.9077345836840529,
    1.5572964573334291,
)
ANGLE_FIT = tuple(
    c * math.sqrt(2.0) * math.sqrt(0.5) ** (len(ACOS_FIT) - 1 - i) for i, c in enumerate(ACOS_FIT)
)


def shade(east, north, east_scale):
    neg_east = east * east_scale
    neg_north = north * (-1.0 / (8.0 * SCALES))
    squared = neg_east * neg_east + neg_north * neg_north
    inverse = lax.rsqrt(1.0 + squared)
    facing_east = neg_east * inverse
    facing_north = neg_north * inverse
    shading = jnp.maximum(inverse * (0.5 * (neg_north - neg_east) + LIGHT_UP), 0.0)
    sine = squared * lax.rsqrt(jnp.maximum(squared, TINY)) * inverse
    cos_one = 1.0 + inverse
    root = lax.rsqrt(cos_one)
    half = cos_one * root
    fit = ANGLE_FIT[0]
    for coefficient in ANGLE_FIT[1:]:
        fit = fit * half + coefficient
    slope = sine * root * fit
    return slope, facing_east, facing_north, shading


def row_scale(row0, total_rows, total_cols):
    row = row0 + lax.broadcasted_iota(jnp.int32, (SUB, LANES), 0)
    turn = (row.astype(jnp.float32) + 0.5) * (1.0 / total_rows)
    angle = jnp.minimum(turn, 1.0 - turn) * math.pi
    power = angle * angle
    sine = jnp.full_like(angle, SINE_FIT[0])
    for coefficient in SINE_FIT[1:]:
        sine = sine * power + coefficient
    spacing = angle * sine * (2.0 * total_rows / total_cols)
    return -1.0 / (8.0 * SCALES * spacing)


def stencil(z, park, q, first_row, total, out, held, store, row_count, tiles):
    lane = lax.broadcasted_iota(jnp.int32, (SUB, LANES), 1)
    lags = [2**k for k in range(SCALES)]

    def steps(lag):
        return -(-lag // SUB)

    def new_boxes(base, active, tile_cache):
        here = [z[j, pl.ds(base + HALO, SUB), :] for j in range(tiles + 1)]
        for k in active:
            s = lags[k]
            pairs = []
            for j in range(tiles + 1):
                pair = z[j, pl.ds(base + HALO + s, SUB), :] + here[j]
                pair = pair * (1.0 / s) if k else pair
                park[k, j] = pair
                pairs.append(pair)
            if 2 * s == LANES:
                halves = [
                    pltpu.roll(jnp.where(lane >= s, pairs[j], pairs[(j + 1) % (tiles + 1)]), s, 1)
                    for j in range(tiles + 1)
                ]
            for j in range(tiles):
                before, after = pairs[(j - 1) % (tiles + 1)], pairs[j + 1]
                if 2 * s == LANES:
                    west, east = halves[(j - 1) % (tiles + 1)], halves[j]
                else:
                    west = pltpu.roll(jnp.where(lane < LANES - s, pairs[j], before), s, 1)
                    east = pltpu.roll(jnp.where(lane >= s, pairs[j], after), LANES - s, 1)
                low, high = park[k, j] + west, park[k, j] + east
                old = tile_cache.get("old") is not None
                if s < SUB:
                    q[k][0, j, pl.ds(base + s + SUB, SUB), :] = low
                    q[k][1, j, pl.ds(base + s + SUB, SUB), :] = high
                    if old:
                        before = q[k][0, j, pl.ds(base + SUB, SUB), :]
                        after = q[k][1, j, pl.ds(base + SUB, SUB), :]
                else:
                    slot = lax.bitwise_and(base // SUB, s // SUB - 1)
                    row = pl.multiple_of(slot * SUB, SUB)
                    if old:
                        before = q[k][0, j, pl.ds(row, SUB), :]
                        after = q[k][1, j, pl.ds(row, SUB), :]
                    q[k][0, j, pl.ds(row, SUB), :] = low
                    q[k][1, j, pl.ds(row, SUB), :] = high
                if old:
                    tile_cache[j, k] = (low, high, before, after)

    def warm(step, active):
        new_boxes(step * SUB, active, {})

    edges = sorted({-steps(s) for s in lags}) + [0]
    for first, last in zip(edges[:-1], edges[1:]):
        active = [k for k, s in enumerate(lags) if -steps(s) <= first]

        @pl.loop(first, last)
        def _(step, active=active):
            warm(step, active)

    def sums(step):
        base = pl.multiple_of(step * SUB, SUB)
        cache = {"old": True}
        new_boxes(base, range(SCALES), cache)
        for j in range(tiles):
            falling = rising = None
            for k in range(SCALES):
                low, high, old_low, old_high = cache[j, k]
                down, up = old_high - low, high - old_low
                falling = down if falling is None else falling + down
                rising = up if rising is None else rising + up
            held[0, j] = falling + rising
            held[1, j] = falling - rising

    def finish(step):
        base = pl.multiple_of(step * SUB, SUB)
        east_scale = row_scale(first_row + base, *total)
        for j in range(tiles):
            results = shade(held[0, j], held[1, j], east_scale)
            for n, value in enumerate(results):
                out[n, pl.ds(base, SUB), j * LANES : (j + 1) * LANES] = value

    count = row_count // SUB

    @pl.loop(0, count, unroll=2)
    def _(step):
        finish(jnp.maximum(step - 1, 0))
        sums(step)

        @pl.when(step > 0)
        def _():
            for copy in store(step - 1):
                copy.start()

    finish(count - 1)
    for copy in store(count - 1):
        copy.start()


def column_copies(source, row0, rows, z, z_row0, first, count, sem):
    return [
        pltpu.make_async_copy(
            source.at[pl.ds(row0, rows), j * LANES : (j + 1) * LANES],
            z.at[first + j, pl.ds(z_row0, rows), :],
            sem.at[first + j],
        )
        for j in range(count)
    ]


def row_copies(out, targets, out_row, row0, rows, sem):
    slope, facing, shading = targets
    places = (slope, facing.at[0], facing.at[1], shading)
    return [
        pltpu.make_async_copy(
            out.at[n, pl.ds(out_row, rows), :], place.at[pl.ds(row0, rows), :], sem.at[n]
        )
        for n, place in enumerate(places)
    ]


def run(copies):
    for copy in copies:
        copy.start()
    for copy in copies:
        copy.wait()


def write_rows(z, park, q, held, out, sem, targets, row0, lat, total, rows, out_rows, tiles):
    def store(step):
        base = pl.multiple_of(step * SUB, SUB)
        return row_copies(out, targets, base, pl.multiple_of(row0 + base, SUB), SUB, sem)

    stencil(z, park, q, lat * rows + row0, total, out, held, store, out_rows, tiles)
    for copy in row_copies(out, targets, 0, row0, out_rows, sem):
        copy.wait()


def main_kernel(rows, tiles, total, x, lon, near, slope, facing, shading, *scratch):
    z, out, held, sem_x, sem_near, sem_out = scratch[:6]
    lat = lax.axis_index("lat")
    odd = lax.rem(lat, 2)
    own = pl.multiple_of(odd * HALO, HALO)
    beyond = pl.multiple_of((1 - odd) * rows, HALO)
    row0 = pl.multiple_of((1 - odd) * HALO, HALO)
    run(
        column_copies(x, 0, rows, z, own, 0, tiles, sem_x)
        + column_copies(lon, 0, rows, z, own, tiles, 1, sem_x)
        + column_copies(near, 0, HALO, z, beyond, 0, tiles + 1, sem_near)
    )
    write_rows(
        z, scratch[6], scratch[7:], held, out, sem_out, (slope, facing, shading), row0, lat, total, rows,
        rows - HALO, tiles,
    )


def rim_kernel(
    rows, tiles, total, lat_count, x, lon, far, far_lon, _a, _b, _c, slope, facing, shading, *scratch
):
    z, out, held, sem_x, sem_far, sem_out = scratch[:6]
    lat = lax.axis_index("lat")
    odd = lax.rem(lat, 2)
    span = 2 * HALO
    own = pl.multiple_of((1 - odd) * HALO, HALO)
    beyond = pl.multiple_of(odd * span, HALO)
    first = pl.multiple_of(odd * (rows - span), HALO)
    row0 = pl.multiple_of(odd * (rows - HALO), HALO)
    run(
        column_copies(x, first, span, z, own, 0, tiles, sem_x)
        + column_copies(lon, first, span, z, own, tiles, 1, sem_x)
        + column_copies(far, 0, HALO, z, beyond, 0, tiles, sem_far)
        + column_copies(far_lon, 0, HALO, z, beyond, tiles, 1, sem_far)
    )

    @pl.when(lat == 0)
    def _():
        for j in range(tiles + 1):
            z[j, 0:HALO, :] = jnp.broadcast_to(z[j, HALO : HALO + 1, :], (HALO, LANES))

    @pl.when(lat == lat_count - 1)
    def _():
        for j in range(tiles + 1):
            z[j, span:, :] = jnp.broadcast_to(z[j, span - 1 : span, :], (HALO, LANES))

    write_rows(
        z, scratch[6], scratch[7:], held, out, sem_out, (slope, facing, shading), row0, lat, total, rows,
        HALO, tiles,
    )


def scratch_for(out_rows, tiles):
    return [
        pltpu.VMEM((tiles + 1, out_rows + 2 * HALO, LANES), jnp.float32),
        pltpu.VMEM((4, out_rows, tiles * LANES), jnp.float32),
        pltpu.VMEM((2, tiles, SUB, LANES), jnp.float32),
        pltpu.SemaphoreType.DMA((tiles + 1,)),
        pltpu.SemaphoreType.DMA((tiles + 1,)),
        pltpu.SemaphoreType.DMA((4,)),
        pltpu.VMEM((SCALES, tiles + 1, SUB, LANES), jnp.float32),
    ] + [
        pltpu.VMEM((2, tiles, out_rows + 3 * SUB if 2**k < SUB else 2**k, LANES), jnp.float32)
        for k in range(SCALES)
    ]


def cost(out_rows, cols):
    cells = out_rows * cols
    return pl.CostEstimate(flops=200 * cells, bytes_accessed=24 * cells, transcendentals=3 * cells)


def lon_halo(x):
    count = lax.axis_size("lon")
    cols = x.shape[1]
    if count == 2:
        lane = lax.broadcasted_iota(jnp.int32, (x.shape[0], LANES), 1)
        both = jnp.where(lane < HALO, x[:, :LANES], x[:, cols - LANES :])
        return lax.ppermute(both, "lon", [(0, 1), (1, 0)])
    westward = [(i, (i - 1) % count) for i in range(count)]
    eastward = [(i, (i + 1) % count) for i in range(count)]
    east = lax.ppermute(x[:, :HALO], "lon", westward)
    west = lax.ppermute(x[:, cols - HALO :], "lon", eastward)
    return jnp.concatenate([east, west], axis=1)


def pairs(first, count):
    ends = [(i, i + 1) for i in range(first, count - 1, 2)]
    return ends + [(b, a) for a, b in ends]


def local(x):
    rows, cols = x.shape
    tiles = cols // LANES
    lat = lax.axis_index("lat")
    count = lax.axis_size("lat")
    odd = lax.rem(lat, 2)
    far_row = odd * (rows - HALO)
    near_row = (1 - odd) * (rows - HALO)

    far_block = lax.dynamic_slice(x, (far_row, 0), (HALO, cols))
    far = lax.ppermute(far_block, "lat", pairs(1, count))
    lon = lon_halo(x)
    near_block = jnp.concatenate(
        [
            lax.dynamic_slice(x, (near_row, 0), (HALO, cols)),
            lax.dynamic_slice(lon, (near_row, 0), (HALO, LANES)),
        ],
        axis=1,
    )
    near = lax.ppermute(near_block, "lat", pairs(0, count))
    corner_block = lax.dynamic_slice(lon, (far_row, 0), (HALO, LANES))
    far_lon = lax.ppermute(corner_block, "lat", pairs(1, count))

    total = (rows * count, cols * lax.axis_size("lon"))
    shapes = [
        jax.ShapeDtypeStruct((rows, cols), jnp.float32),
        jax.ShapeDtypeStruct((2, rows, cols), jnp.float32),
        jax.ShapeDtypeStruct((rows, cols), jnp.float32),
    ]
    hbm = pl.BlockSpec(memory_space=pltpu.HBM)
    halo = pl.BlockSpec(memory_space=HALO_SPACE)
    outs = pl.pallas_call(
        functools.partial(main_kernel, rows, tiles, total),
        out_shape=shapes,
        in_specs=[hbm, halo, halo],
        out_specs=[hbm] * 3,
        scratch_shapes=scratch_for(rows - HALO, tiles),
        cost_estimate=cost(rows - HALO, cols),
        compiler_params=pltpu.CompilerParams(vmem_limit_bytes=VMEM_LIMIT),
        name="stencil_main",
    )(x, lon, near)
    return tuple(
        pl.pallas_call(
            functools.partial(rim_kernel, rows, tiles, total, count),
            out_shape=shapes,
            in_specs=[hbm] + [halo] * 3 + [hbm] * 3,
            out_specs=[hbm] * 3,
            input_output_aliases={4: 0, 5: 1, 6: 2},
            scratch_shapes=scratch_for(HALO, tiles),
            cost_estimate=cost(HALO, cols),
            compiler_params=pltpu.CompilerParams(vmem_limit_bytes=VMEM_LIMIT),
            name="stencil_rim",
        )(x, lon, far, far_lon, *outs)
    )


def solution(mesh):
    in_specs = (P("lat", "lon"),)
    out_specs = (P("lat", "lon"), P(None, "lat", "lon"), P("lat", "lon"))

    return jax.shard_map(local, mesh=mesh, in_specs=in_specs, out_specs=out_specs, check_vma=False)
```

```python
import functools
import math

import jax
import jax.numpy as jnp
from jax import lax
from jax.experimental import pallas as pl
from jax.experimental.pallas import tpu as pltpu
from jax.sharding import PartitionSpec as P


SCALES = 7
HALO = 64
LANES = 128
SUB = 8
VMEM_LIMIT = 48 * 2**20
HALO_SPACE = pltpu.VMEM

LIGHT_UP = math.sqrt(0.5)
TINY = 1.17549435e-38

SINE_FIT = tuple((-1.0) ** k / math.factorial(2 * k + 1) for k in range(7, -1, -1))
ACOS_FIT = (
    0.036142768221257435,
    -0.1987486877325598,
    0.5130441168137142,
    -0.9077345836840529,
    1.5572964573334291,
)
ANGLE_FIT = tuple(
    c * math.sqrt(2.0) * math.sqrt(0.5) ** (len(ACOS_FIT) - 1 - i) for i, c in enumerate(ACOS_FIT)
)


def shade(east, north, east_scale):
    neg_east = east * east_scale
    neg_north = north * (-1.0 / (8.0 * SCALES))
    squared = neg_east * neg_east + neg_north * neg_north
    inverse = lax.rsqrt(1.0 + squared)
    facing_east = neg_east * inverse
    facing_north = neg_north * inverse
    shading = jnp.maximum(inverse * (0.5 * (neg_north - neg_east) + LIGHT_UP), 0.0)
    sine = squared * lax.rsqrt(jnp.maximum(squared, TINY)) * inverse
    cos_one = 1.0 + inverse
    root = lax.rsqrt(cos_one)
    half = cos_one * root
    fit = ANGLE_FIT[0]
    for coefficient in ANGLE_FIT[1:]:
        fit = fit * half + coefficient
    slope = sine * root * fit
    return slope, facing_east, facing_north, shading


def row_scale(row0, total_rows, total_cols):
    row = row0 + lax.broadcasted_iota(jnp.int32, (SUB, LANES), 0)
    turn = (row.astype(jnp.float32) + 0.5) * (1.0 / total_rows)
    angle = jnp.minimum(turn, 1.0 - turn) * math.pi
    power = angle * angle
    sine = jnp.full_like(angle, SINE_FIT[0])
    for coefficient in SINE_FIT[1:]:
        sine = sine * power + coefficient
    spacing = angle * sine * (2.0 * total_rows / total_cols)
    return -1.0 / (8.0 * SCALES * spacing)


def stencil(z, park, q, first_row, total, out, held, store, row_count, tiles):
    lane = lax.broadcasted_iota(jnp.int32, (SUB, LANES), 1)
    lags = [2**k for k in range(SCALES)]

    def steps(lag):
        return -(-lag // SUB)

    def new_boxes(base, active, tile_cache):
        here = [z[j, pl.ds(base + HALO, SUB), :] for j in range(tiles + 1)]
        for k in active:
            s = lags[k]
            pairs = []
            for j in range(tiles + 1):
                pair = z[j, pl.ds(base + HALO + s, SUB), :] + here[j]
                pair = pair * (1.0 / s) if k else pair
                park[k, j] = pair
                pairs.append(pair)
            if 2 * s == LANES:
                halves = [
                    pltpu.roll(jnp.where(lane >= s, pairs[j], pairs[(j + 1) % (tiles + 1)]), s, 1)
                    for j in range(tiles + 1)
                ]
            for j in range(tiles):
                before, after = pairs[(j - 1) % (tiles + 1)], pairs[j + 1]
                if 2 * s == LANES:
                    west, east = halves[(j - 1) % (tiles + 1)], halves[j]
                else:
                    west = pltpu.roll(jnp.where(lane < LANES - s, pairs[j], before), s, 1)
                    east = pltpu.roll(jnp.where(lane >= s, pairs[j], after), LANES - s, 1)
                low, high = park[k, j] + west, park[k, j] + east
                old = tile_cache.get("old") is not None
                if s < SUB:
                    q[k][0, j, pl.ds(base + s + SUB, SUB), :] = low
                    q[k][1, j, pl.ds(base + s + SUB, SUB), :] = high
                    if old:
                        before = q[k][0, j, pl.ds(base + SUB, SUB), :]
                        after = q[k][1, j, pl.ds(base + SUB, SUB), :]
                else:
                    slot = lax.bitwise_and(base // SUB, s // SUB - 1)
                    row = pl.multiple_of(slot * SUB, SUB)
                    if old:
                        before = q[k][0, j, pl.ds(row, SUB), :]
                        after = q[k][1, j, pl.ds(row, SUB), :]
                    q[k][0, j, pl.ds(row, SUB), :] = low
                    q[k][1, j, pl.ds(row, SUB), :] = high
                if old:
                    tile_cache[j, k] = (low, high, before, after)

    def warm(step, active):
        new_boxes(step * SUB, active, {})

    edges = sorted({-steps(s) for s in lags}) + [0]
    for first, last in zip(edges[:-1], edges[1:]):
        active = [k for k, s in enumerate(lags) if -steps(s) <= first]

        @pl.loop(first, last)
        def _(step, active=active):
            warm(step, active)

    def sums(step):
        base = pl.multiple_of(step * SUB, SUB)
        cache = {"old": True}
        new_boxes(base, range(SCALES), cache)
        for j in range(tiles):
            falling = rising = None
            for k in range(SCALES):
                low, high, old_low, old_high = cache[j, k]
                down, up = old_high - low, high - old_low
                falling = down if falling is None else falling + down
                rising = up if rising is None else rising + up
            held[0, j] = falling + rising
            held[1, j] = falling - rising

    def finish(step):
        base = pl.multiple_of(step * SUB, SUB)
        east_scale = row_scale(first_row + base, *total)
        for j in range(tiles):
            results = shade(held[0, j], held[1, j], east_scale)
            for n, value in enumerate(results):
                out[n, pl.ds(base, SUB), j * LANES : (j + 1) * LANES] = value

    count = row_count // SUB

    @pl.loop(0, count, unroll=4)
    def _(step):
        finish(jnp.maximum(step - 1, 0))
        sums(step)

        @pl.when(step > 0)
        def _():
            for copy in store(step - 1):
                copy.start()

    finish(count - 1)
    for copy in store(count - 1):
        copy.start()


def column_copies(source, row0, rows, z, z_row0, first, count, sem):
    return [
        pltpu.make_async_copy(
            source.at[pl.ds(row0, rows), j * LANES : (j + 1) * LANES],
            z.at[first + j, pl.ds(z_row0, rows), :],
            sem.at[first + j],
        )
        for j in range(count)
    ]


def tile_copy(source, row0, rows, z, z_row0, tile, sem):
    return pltpu.make_async_copy(
        source.at[pl.ds(pl.multiple_of(row0, HALO), rows), :],
        z.at[tile, pl.ds(pl.multiple_of(z_row0, HALO), rows), :],
        sem,
    )


def row_copies(out, targets, out_row, row0, rows, sem):
    slope, facing, shading = targets
    places = (slope, facing.at[0], facing.at[1], shading)
    return [
        pltpu.make_async_copy(
            out.at[n, pl.ds(out_row, rows), :], place.at[pl.ds(row0, rows), :], sem.at[n]
        )
        for n, place in enumerate(places)
    ]


def run(copies):
    for copy in copies:
        copy.start()
    for copy in copies:
        copy.wait()


def write_rows(z, park, q, held, out, sem, targets, row0, lat, total, rows, out_rows, tiles):
    def store(step):
        base = pl.multiple_of(step * SUB, SUB)
        return row_copies(out, targets, base, pl.multiple_of(row0 + base, SUB), SUB, sem)

    stencil(z, park, q, lat * rows + row0, total, out, held, store, out_rows, tiles)
    for copy in row_copies(out, targets, 0, row0, out_rows, sem):
        copy.wait()


def main_kernel(rows, tiles, total, x, lon_rim, lon_mid, near, slope, facing, shading, *scratch):
    z, out, held, sem_x, sem_lon, sem_near, sem_out = scratch[:7]
    lat = lax.axis_index("lat")
    odd = lax.rem(lat, 2)
    own = pl.multiple_of(odd * HALO, HALO)
    beyond = pl.multiple_of((1 - odd) * rows, HALO)
    row0 = pl.multiple_of((1 - odd) * HALO, HALO)
    mid = rows - 2 * HALO
    run(
        column_copies(x, 0, rows, z, own, 0, tiles, sem_x)
        + [
            tile_copy(lon_rim, 0, HALO, z, own, tiles, sem_lon.at[0]),
            tile_copy(lon_mid, 0, mid, z, own + HALO, tiles, sem_lon.at[1]),
            tile_copy(lon_rim, HALO, HALO, z, own + HALO + mid, tiles, sem_lon.at[2]),
        ]
        + column_copies(near, 0, HALO, z, beyond, 0, tiles + 1, sem_near)
    )
    write_rows(
        z, scratch[7], scratch[8:], held, out, sem_out, (slope, facing, shading), row0, lat, total,
        rows, rows - HALO, tiles,
    )


def rim_kernel(
    rows, tiles, total, lat_count, x, lon_rim, lon_mid, far, _a, _b, _c, slope, facing, shading,
    *scratch,
):
    z, out, held, sem_x, sem_lon, sem_far, sem_out = scratch[:7]
    lat = lax.axis_index("lat")
    odd = lax.rem(lat, 2)
    span = 2 * HALO
    own = pl.multiple_of((1 - odd) * HALO, HALO)
    beyond = pl.multiple_of(odd * span, HALO)
    first = pl.multiple_of(odd * (rows - span), HALO)
    row0 = pl.multiple_of(odd * (rows - HALO), HALO)
    edge = pl.multiple_of(odd * HALO, HALO)
    mid = pl.multiple_of(odd * (rows - 3 * HALO), HALO)
    run(
        column_copies(x, first, span, z, own, 0, tiles, sem_x)
        + [
            tile_copy(lon_rim, edge, HALO, z, own + edge, tiles, sem_lon.at[0]),
            tile_copy(lon_mid, mid, HALO, z, own + HALO - edge, tiles, sem_lon.at[1]),
        ]
        + column_copies(far, 0, HALO, z, beyond, 0, tiles + 1, sem_far)
    )

    @pl.when(lat == 0)
    def _():
        for j in range(tiles + 1):
            z[j, 0:HALO, :] = jnp.broadcast_to(z[j, HALO : HALO + 1, :], (HALO, LANES))

    @pl.when(lat == lat_count - 1)
    def _():
        for j in range(tiles + 1):
            z[j, span:, :] = jnp.broadcast_to(z[j, span - 1 : span, :], (HALO, LANES))

    write_rows(
        z, scratch[7], scratch[8:], held, out, sem_out, (slope, facing, shading), row0, lat, total,
        rows, HALO, tiles,
    )


def scratch_for(out_rows, tiles):
    return [
        pltpu.VMEM((tiles + 1, out_rows + 2 * HALO, LANES), jnp.float32),
        pltpu.VMEM((4, out_rows, tiles * LANES), jnp.float32),
        pltpu.VMEM((2, tiles, SUB, LANES), jnp.float32),
        pltpu.SemaphoreType.DMA((tiles,)),
        pltpu.SemaphoreType.DMA((3,)),
        pltpu.SemaphoreType.DMA((tiles + 1,)),
        pltpu.SemaphoreType.DMA((4,)),
        pltpu.VMEM((SCALES, tiles + 1, SUB, LANES), jnp.float32),
    ] + [
        pltpu.VMEM((2, tiles, out_rows + 3 * SUB if 2**k < SUB else 2**k, LANES), jnp.float32)
        for k in range(SCALES)
    ]


def cost(out_rows, cols):
    cells = out_rows * cols
    return pl.CostEstimate(flops=200 * cells, bytes_accessed=24 * cells, transcendentals=3 * cells)


def lon_halo(first, last):
    count = lax.axis_size("lon")
    if count == 2:
        lane = lax.broadcasted_iota(jnp.int32, first.shape, 1)
        both = jnp.where(lane < HALO, first, last)
        return lax.ppermute(both, "lon", [(0, 1), (1, 0)])
    westward = [(i, (i - 1) % count) for i in range(count)]
    eastward = [(i, (i + 1) % count) for i in range(count)]
    east = lax.ppermute(first[:, :HALO], "lon", westward)
    west = lax.ppermute(last[:, LANES - HALO :], "lon", eastward)
    return jnp.concatenate([east, west], axis=1)


def pairs(first, count):
    ends = [(i, i + 1) for i in range(first, count - 1, 2)]
    return ends + [(b, a) for a, b in ends]


def local(x):
    rows, cols = x.shape
    tiles = cols // LANES
    lat = lax.axis_index("lat")
    count = lax.axis_size("lat")
    odd = lax.rem(lat, 2)

    def both_rims(part):
        return jnp.concatenate([part[:HALO], part[rows - HALO :]], axis=0)

    def rim(start):
        return jnp.concatenate(
            [
                lax.dynamic_slice(x, (start * (rows - HALO), 0), (HALO, cols)),
                lax.dynamic_slice(lon_rim, (start * HALO, 0), (HALO, LANES)),
            ],
            axis=1,
        )

    first, last = x[:, :LANES], x[:, cols - LANES :]
    lon_rim = lon_halo(both_rims(first), both_rims(last))
    lon_mid = lon_halo(first[HALO : rows - HALO], last[HALO : rows - HALO])
    far = lax.ppermute(rim(odd), "lat", pairs(1, count))
    near = lax.ppermute(rim(1 - odd), "lat", pairs(0, count))

    total = (rows * count, cols * lax.axis_size("lon"))
    shapes = [
        jax.ShapeDtypeStruct((rows, cols), jnp.float32),
        jax.ShapeDtypeStruct((2, rows, cols), jnp.float32),
        jax.ShapeDtypeStruct((rows, cols), jnp.float32),
    ]
    hbm = pl.BlockSpec(memory_space=pltpu.HBM)
    halo = pl.BlockSpec(memory_space=HALO_SPACE)
    outs = pl.pallas_call(
        functools.partial(main_kernel, rows, tiles, total),
        out_shape=shapes,
        in_specs=[hbm] + [halo] * 3,
        out_specs=[hbm] * 3,
        scratch_shapes=scratch_for(rows - HALO, tiles),
        cost_estimate=cost(rows - HALO, cols),
        compiler_params=pltpu.CompilerParams(vmem_limit_bytes=VMEM_LIMIT),
        name="stencil_main",
    )(x, lon_rim, lon_mid, near)
    return tuple(
        pl.pallas_call(
            functools.partial(rim_kernel, rows, tiles, total, count),
            out_shape=shapes,
            in_specs=[hbm] + [halo] * 3 + [hbm] * 3,
            out_specs=[hbm] * 3,
            input_output_aliases={4: 0, 5: 1, 6: 2},
            scratch_shapes=scratch_for(HALO, tiles),
            cost_estimate=cost(HALO, cols),
            compiler_params=pltpu.CompilerParams(vmem_limit_bytes=VMEM_LIMIT),
            name="stencil_rim",
        )(x, lon_rim, lon_mid, far, *outs)
    )


def solution(mesh):
    in_specs = (P("lat", "lon"),)
    out_specs = (P("lat", "lon"), P(None, "lat", "lon"), P("lat", "lon"))

    return jax.shard_map(local, mesh=mesh, in_specs=in_specs, out_specs=out_specs, check_vma=False)
```

```python
import functools
import math

import jax
import jax.numpy as jnp
from jax import lax
from jax.experimental import pallas as pl
from jax.experimental.pallas import tpu as pltpu
from jax.sharding import PartitionSpec as P


SCALES = 7
HALO = 64
LANES = 128
SUB = 8
VMEM_LIMIT = 48 * 2**20
HALO_SPACE = pltpu.VMEM

LIGHT_UP = math.sqrt(0.5)
TINY = 1.17549435e-38

SINE_FIT = tuple((-1.0) ** k / math.factorial(2 * k + 1) for k in range(7, -1, -1))
ACOS_FIT = (
    0.036142768221257435,
    -0.1987486877325598,
    0.5130441168137142,
    -0.9077345836840529,
    1.5572964573334291,
)
ANGLE_FIT = tuple(
    c * math.sqrt(2.0) * math.sqrt(0.5) ** (len(ACOS_FIT) - 1 - i) for i, c in enumerate(ACOS_FIT)
)


def shade(east, north, east_scale):
    neg_east = east * east_scale
    neg_north = north * (-1.0 / (8.0 * SCALES))
    squared = neg_east * neg_east + neg_north * neg_north
    inverse = lax.rsqrt(1.0 + squared)
    facing_east = neg_east * inverse
    facing_north = neg_north * inverse
    shading = jnp.maximum(inverse * (0.5 * (neg_north - neg_east) + LIGHT_UP), 0.0)
    sine = squared * lax.rsqrt(jnp.maximum(squared, TINY)) * inverse
    cos_one = 1.0 + inverse
    root = lax.rsqrt(cos_one)
    half = cos_one * root
    fit = ANGLE_FIT[0]
    for coefficient in ANGLE_FIT[1:]:
        fit = fit * half + coefficient
    slope = sine * root * fit
    return slope, facing_east, facing_north, shading


def row_scale(row0, total_rows, total_cols):
    row = row0 + lax.broadcasted_iota(jnp.int32, (SUB, LANES), 0)
    turn = (row.astype(jnp.float32) + 0.5) * (1.0 / total_rows)
    angle = jnp.minimum(turn, 1.0 - turn) * math.pi
    power = angle * angle
    sine = jnp.full_like(angle, SINE_FIT[0])
    for coefficient in SINE_FIT[1:]:
        sine = sine * power + coefficient
    spacing = angle * sine * (2.0 * total_rows / total_cols)
    return -1.0 / (8.0 * SCALES * spacing)


def stencil(z, park, q, first_row, total, out, held, store, row_count, tiles):
    lane = lax.broadcasted_iota(jnp.int32, (SUB, LANES), 1)
    lags = [2**k for k in range(SCALES)]

    def steps(lag):
        return -(-lag // SUB)

    def new_boxes(base, active, tile_cache):
        here = [z[j, pl.ds(base + HALO, SUB), :] for j in range(tiles + 1)]
        for k in active:
            s = lags[k]
            pairs = []
            for j in range(tiles + 1):
                pair = z[j, pl.ds(base + HALO + s, SUB), :] + here[j]
                pair = pair * (1.0 / s) if k else pair
                park[k, j] = pair
                pairs.append(pair)
            if 2 * s == LANES:
                halves = [
                    pltpu.roll(jnp.where(lane >= s, pairs[j], pairs[(j + 1) % (tiles + 1)]), s, 1)
                    for j in range(tiles + 1)
                ]
            for j in range(tiles):
                before, after = pairs[(j - 1) % (tiles + 1)], pairs[j + 1]
                if 2 * s == LANES:
                    west, east = halves[(j - 1) % (tiles + 1)], halves[j]
                else:
                    west = pltpu.roll(jnp.where(lane < LANES - s, pairs[j], before), s, 1)
                    east = pltpu.roll(jnp.where(lane >= s, pairs[j], after), LANES - s, 1)
                low, high = park[k, j] + west, park[k, j] + east
                old = tile_cache.get("old") is not None
                if s < SUB:
                    q[k][0, j, pl.ds(base + s + SUB, SUB), :] = low
                    q[k][1, j, pl.ds(base + s + SUB, SUB), :] = high
                    if old:
                        before = q[k][0, j, pl.ds(base + SUB, SUB), :]
                        after = q[k][1, j, pl.ds(base + SUB, SUB), :]
                else:
                    slot = lax.bitwise_and(base // SUB, s // SUB - 1)
                    row = pl.multiple_of(slot * SUB, SUB)
                    if old:
                        before = q[k][0, j, pl.ds(row, SUB), :]
                        after = q[k][1, j, pl.ds(row, SUB), :]
                    q[k][0, j, pl.ds(row, SUB), :] = low
                    q[k][1, j, pl.ds(row, SUB), :] = high
                if old:
                    tile_cache[j, k] = (low, high, before, after)

    def warm(step, active):
        new_boxes(step * SUB, active, {})

    edges = sorted({-steps(s) for s in lags}) + [0]
    for first, last in zip(edges[:-1], edges[1:]):
        active = [k for k, s in enumerate(lags) if -steps(s) <= first]

        @pl.loop(first, last, unroll=last - first)
        def _(step, active=active):
            warm(step, active)

    def sums(step):
        base = pl.multiple_of(step * SUB, SUB)
        cache = {"old": True}
        new_boxes(base, range(SCALES), cache)
        for j in range(tiles):
            falling = rising = None
            for k in range(SCALES):
                low, high, old_low, old_high = cache[j, k]
                down, up = old_high - low, high - old_low
                falling = down if falling is None else falling + down
                rising = up if rising is None else rising + up
            held[0, j] = falling + rising
            held[1, j] = falling - rising

    def finish(step):
        base = pl.multiple_of(step * SUB, SUB)
        east_scale = row_scale(first_row + base, *total)
        for j in range(tiles):
            results = shade(held[0, j], held[1, j], east_scale)
            for n, value in enumerate(results):
                out[n, pl.ds(base, SUB), j * LANES : (j + 1) * LANES] = value

    count = row_count // SUB

    @pl.loop(0, count, unroll=4)
    def _(step):
        finish(jnp.maximum(step - 1, 0))
        sums(step)

        @pl.when(step > 0)
        def _():
            for copy in store(step - 1):
                copy.start()

    finish(count - 1)
    for copy in store(count - 1):
        copy.start()


def column_copies(source, row0, rows, z, z_row0, first, count, sem):
    return [
        pltpu.make_async_copy(
            source.at[pl.ds(row0, rows), j * LANES : (j + 1) * LANES],
            z.at[first + j, pl.ds(z_row0, rows), :],
            sem.at[first + j],
        )
        for j in range(count)
    ]


def row_copies(out, targets, out_row, row0, rows, sem):
    slope, facing, shading = targets
    places = (slope, facing.at[0], facing.at[1], shading)
    return [
        pltpu.make_async_copy(
            out.at[n, pl.ds(out_row, rows), :], place.at[pl.ds(row0, rows), :], sem.at[n]
        )
        for n, place in enumerate(places)
    ]


def run(copies):
    for copy in copies:
        copy.start()
    for copy in copies:
        copy.wait()


def write_rows(z, park, q, held, out, sem, targets, row0, lat, total, rows, out_rows, tiles):
    def store(step):
        base = pl.multiple_of(step * SUB, SUB)
        return row_copies(out, targets, base, pl.multiple_of(row0 + base, SUB), SUB, sem)

    stencil(z, park, q, lat * rows + row0, total, out, held, store, out_rows, tiles)
    for copy in row_copies(out, targets, 0, row0, out_rows, sem):
        copy.wait()


def main_kernel(rows, tiles, total, x, lon, near, slope, facing, shading, *scratch):
    z, out, held, sem_x, sem_near, sem_out = scratch[:6]
    lat = lax.axis_index("lat")
    odd = lax.rem(lat, 2)
    own = pl.multiple_of(odd * HALO, HALO)
    beyond = pl.multiple_of((1 - odd) * rows, HALO)
    row0 = pl.multiple_of((1 - odd) * HALO, HALO)
    run(
        column_copies(x, 0, rows, z, own, 0, tiles, sem_x)
        + column_copies(lon, 0, rows, z, own, tiles, 1, sem_x)
        + column_copies(near, 0, HALO, z, beyond, 0, tiles + 1, sem_near)
    )
    write_rows(
        z, scratch[6], scratch[7:], held, out, sem_out, (slope, facing, shading), row0, lat, total, rows,
        rows - HALO, tiles,
    )


def rim_kernel(
    rows, tiles, total, lat_count, x, lon, far, far_lon, _a, _b, _c, slope, facing, shading, *scratch
):
    z, out, held, sem_x, sem_far, sem_out = scratch[:6]
    lat = lax.axis_index("lat")
    odd = lax.rem(lat, 2)
    span = 2 * HALO
    own = pl.multiple_of((1 - odd) * HALO, HALO)
    beyond = pl.multiple_of(odd * span, HALO)
    first = pl.multiple_of(odd * (rows - span), HALO)
    row0 = pl.multiple_of(odd * (rows - HALO), HALO)
    run(
        column_copies(x, first, span, z, own, 0, tiles, sem_x)
        + column_copies(lon, first, span, z, own, tiles, 1, sem_x)
        + column_copies(far, 0, HALO, z, beyond, 0, tiles, sem_far)
        + column_copies(far_lon, 0, HALO, z, beyond, tiles, 1, sem_far)
    )

    @pl.when(lat == 0)
    def _():
        for j in range(tiles + 1):
            z[j, 0:HALO, :] = jnp.broadcast_to(z[j, HALO : HALO + 1, :], (HALO, LANES))

    @pl.when(lat == lat_count - 1)
    def _():
        for j in range(tiles + 1):
            z[j, span:, :] = jnp.broadcast_to(z[j, span - 1 : span, :], (HALO, LANES))

    write_rows(
        z, scratch[6], scratch[7:], held, out, sem_out, (slope, facing, shading), row0, lat, total, rows,
        HALO, tiles,
    )


def scratch_for(out_rows, tiles):
    return [
        pltpu.VMEM((tiles + 1, out_rows + 2 * HALO, LANES), jnp.float32),
        pltpu.VMEM((4, out_rows, tiles * LANES), jnp.float32),
        pltpu.VMEM((2, tiles, SUB, LANES), jnp.float32),
        pltpu.SemaphoreType.DMA((tiles + 1,)),
        pltpu.SemaphoreType.DMA((tiles + 1,)),
        pltpu.SemaphoreType.DMA((4,)),
        pltpu.VMEM((SCALES, tiles + 1, SUB, LANES), jnp.float32),
    ] + [
        pltpu.VMEM((2, tiles, out_rows + 3 * SUB if 2**k < SUB else 2**k, LANES), jnp.float32)
        for k in range(SCALES)
    ]


def cost(out_rows, cols):
    cells = out_rows * cols
    return pl.CostEstimate(flops=200 * cells, bytes_accessed=24 * cells, transcendentals=3 * cells)


def lon_halo(sides):
    count = lax.axis_size("lon")
    if count == 2:
        return lax.ppermute(sides, "lon", [(0, 1), (1, 0)])
    westward = [(i, (i - 1) % count) for i in range(count)]
    eastward = [(i, (i + 1) % count) for i in range(count)]
    east = lax.ppermute(sides[:, :HALO], "lon", westward)
    west = lax.ppermute(sides[:, HALO:], "lon", eastward)
    return jnp.concatenate([east, west], axis=1)


def pairs(first, count):
    ends = [(i, i + 1) for i in range(first, count - 1, 2)]
    return ends + [(b, a) for a, b in ends]


def local(x):
    rows, cols = x.shape
    tiles = cols // LANES
    lat = lax.axis_index("lat")
    count = lax.axis_size("lat")
    odd = lax.rem(lat, 2)
    far_row = odd * (rows - HALO)
    near_row = (1 - odd) * (rows - HALO)

    halo = pl.BlockSpec(memory_space=HALO_SPACE)
    hbm = pl.BlockSpec(memory_space=pltpu.HBM)
    far_block = lax.dynamic_slice(x, (far_row, 0), (HALO, cols))
    near_rows = lax.dynamic_slice(x, (near_row, 0), (HALO, cols))
    held_x, far_block, near_rows = lax.optimization_barrier((x, far_block, near_rows))
    lane = lax.broadcasted_iota(jnp.int32, (rows, LANES), 1)
    sides = jnp.where(lane < HALO, held_x[:, :LANES], held_x[:, cols - LANES :])
    lon = lon_halo(sides)
    far = lax.ppermute(far_block, "lat", pairs(1, count))
    near_block = jnp.concatenate(
        [near_rows, lax.dynamic_slice(lon, (near_row, 0), (HALO, LANES))], axis=1
    )
    near = lax.ppermute(near_block, "lat", pairs(0, count))
    corner_block = lax.dynamic_slice(lon, (far_row, 0), (HALO, LANES))
    far_lon = lax.ppermute(corner_block, "lat", pairs(1, count))

    total = (rows * count, cols * lax.axis_size("lon"))
    shapes = [
        jax.ShapeDtypeStruct((rows, cols), jnp.float32),
        jax.ShapeDtypeStruct((2, rows, cols), jnp.float32),
        jax.ShapeDtypeStruct((rows, cols), jnp.float32),
    ]
    outs = pl.pallas_call(
        functools.partial(main_kernel, rows, tiles, total),
        out_shape=shapes,
        in_specs=[hbm, halo, halo],
        out_specs=[hbm] * 3,
        scratch_shapes=scratch_for(rows - HALO, tiles),
        cost_estimate=cost(rows - HALO, cols),
        compiler_params=pltpu.CompilerParams(vmem_limit_bytes=VMEM_LIMIT),
        name="stencil_main",
    )(x, lon, near)
    return tuple(
        pl.pallas_call(
            functools.partial(rim_kernel, rows, tiles, total, count),
            out_shape=shapes,
            in_specs=[hbm] + [halo] * 3 + [hbm] * 3,
            out_specs=[hbm] * 3,
            input_output_aliases={4: 0, 5: 1, 6: 2},
            scratch_shapes=scratch_for(HALO, tiles),
            cost_estimate=cost(HALO, cols),
            compiler_params=pltpu.CompilerParams(vmem_limit_bytes=VMEM_LIMIT),
            name="stencil_rim",
        )(x, lon, far, far_lon, *outs)
    )


def solution(mesh):
    in_specs = (P("lat", "lon"),)
    out_specs = (P("lat", "lon"), P(None, "lat", "lon"), P("lat", "lon"))

    return jax.shard_map(local, mesh=mesh, in_specs=in_specs, out_specs=out_specs, check_vma=False)
```

```python
import functools
import math

import jax
import jax.numpy as jnp
from jax import lax
from jax.experimental import pallas as pl
from jax.experimental.pallas import tpu as pltpu
from jax.sharding import PartitionSpec as P


SCALES = 7
HALO = 64
LANES = 128
SUB = 8
VMEM_LIMIT = 48 * 2**20
HALO_SPACE = pltpu.VMEM

LIGHT_UP = math.sqrt(0.5)
TINY = 1.17549435e-38

SINE_FIT = tuple((-1.0) ** k / math.factorial(2 * k + 1) for k in range(7, -1, -1))
ACOS_FIT = (
    0.036142768221257435,
    -0.1987486877325598,
    0.5130441168137142,
    -0.9077345836840529,
    1.5572964573334291,
)
ANGLE_FIT = tuple(
    c * math.sqrt(2.0) * math.sqrt(0.5) ** (len(ACOS_FIT) - 1 - i) for i, c in enumerate(ACOS_FIT)
)


def shade(east, north, east_scale):
    neg_east = east * east_scale
    neg_north = north * (-1.0 / (8.0 * SCALES))
    squared = neg_east * neg_east + neg_north * neg_north
    inverse = lax.rsqrt(1.0 + squared)
    facing_east = neg_east * inverse
    facing_north = neg_north * inverse
    shading = jnp.maximum(inverse * (0.5 * (neg_north - neg_east) + LIGHT_UP), 0.0)
    sine = squared * lax.rsqrt(jnp.maximum(squared, TINY)) * inverse
    cos_one = 1.0 + inverse
    root = lax.rsqrt(cos_one)
    half = cos_one * root
    fit = ANGLE_FIT[0]
    for coefficient in ANGLE_FIT[1:]:
        fit = fit * half + coefficient
    slope = sine * root * fit
    return slope, facing_east, facing_north, shading


def row_scale(row0, total_rows, total_cols):
    row = row0 + lax.broadcasted_iota(jnp.int32, (SUB, LANES), 0)
    turn = (row.astype(jnp.float32) + 0.5) * (1.0 / total_rows)
    angle = jnp.minimum(turn, 1.0 - turn) * math.pi
    power = angle * angle
    sine = jnp.full_like(angle, SINE_FIT[0])
    for coefficient in SINE_FIT[1:]:
        sine = sine * power + coefficient
    spacing = angle * sine * (2.0 * total_rows / total_cols)
    return -1.0 / (8.0 * SCALES * spacing)


def stencil(z, park, q, first_row, total, out, held, store, row_count, tiles):
    lane = lax.broadcasted_iota(jnp.int32, (SUB, LANES), 1)
    lags = [2**k for k in range(SCALES)]

    def steps(lag):
        return -(-lag // SUB)

    def new_boxes(base, active, tile_cache):
        here = [z[j, pl.ds(base + HALO, SUB), :] for j in range(tiles + 1)]
        for k in active:
            s = lags[k]
            pairs = []
            for j in range(tiles + 1):
                pair = z[j, pl.ds(base + HALO + s, SUB), :] + here[j]
                pair = pair * (1.0 / s) if k else pair
                park[k, j] = pair
                pairs.append(pair)
            if 2 * s == LANES:
                halves = [
                    pltpu.roll(jnp.where(lane >= s, pairs[j], pairs[(j + 1) % (tiles + 1)]), s, 1)
                    for j in range(tiles + 1)
                ]
            for j in range(tiles):
                before, after = pairs[(j - 1) % (tiles + 1)], pairs[j + 1]
                if 2 * s == LANES:
                    west, east = halves[(j - 1) % (tiles + 1)], halves[j]
                else:
                    west = pltpu.roll(jnp.where(lane < LANES - s, pairs[j], before), s, 1)
                    east = pltpu.roll(jnp.where(lane >= s, pairs[j], after), LANES - s, 1)
                low, high = park[k, j] + west, park[k, j] + east
                old = tile_cache.get("old") is not None
                if s < SUB:
                    q[k][0, j, pl.ds(base + s + SUB, SUB), :] = low
                    q[k][1, j, pl.ds(base + s + SUB, SUB), :] = high
                    if old:
                        before = q[k][0, j, pl.ds(base + SUB, SUB), :]
                        after = q[k][1, j, pl.ds(base + SUB, SUB), :]
                else:
                    slot = lax.bitwise_and(base // SUB, s // SUB - 1)
                    row = pl.multiple_of(slot * SUB, SUB)
                    if old:
                        before = q[k][0, j, pl.ds(row, SUB), :]
                        after = q[k][1, j, pl.ds(row, SUB), :]
                    q[k][0, j, pl.ds(row, SUB), :] = low
                    q[k][1, j, pl.ds(row, SUB), :] = high
                if old:
                    down, up = after - low, high - before
                    if j in tile_cache:
                        down, up = tile_cache[j][0] + down, tile_cache[j][1] + up
                    tile_cache[j] = (down, up)

    def warm(step, active):
        new_boxes(step * SUB, active, {})

    edges = sorted({-steps(s) for s in lags}) + [0]
    for first, last in zip(edges[:-1], edges[1:]):
        active = [k for k, s in enumerate(lags) if -steps(s) <= first]

        @pl.loop(first, last, unroll=last - first)
        def _(step, active=active):
            warm(step, active)

    def sums(step):
        base = pl.multiple_of(step * SUB, SUB)
        cache = {"old": True}
        new_boxes(base, range(SCALES), cache)
        for j in range(tiles):
            falling, rising = cache[j]
            held[0, j] = falling + rising
            held[1, j] = falling - rising

    def finish(step):
        base = pl.multiple_of(step * SUB, SUB)
        east_scale = row_scale(first_row + base, *total)
        for j in range(tiles):
            results = shade(held[0, j], held[1, j], east_scale)
            for n, value in enumerate(results):
                out[n, pl.ds(base, SUB), j * LANES : (j + 1) * LANES] = value

    count = row_count // SUB

    @pl.loop(0, count, unroll=8)
    def _(step):
        finish(jnp.maximum(step - 1, 0))
        sums(step)

        @pl.when(step > 0)
        def _():
            for copy in store(step - 1):
                copy.start()

    finish(count - 1)
    for copy in store(count - 1):
        copy.start()


def column_copies(source, row0, rows, z, z_row0, first, count, sem):
    return [
        pltpu.make_async_copy(
            source.at[pl.ds(row0, rows), j * LANES : (j + 1) * LANES],
            z.at[first + j, pl.ds(z_row0, rows), :],
            sem.at[first + j],
        )
        for j in range(count)
    ]


def row_copies(out, targets, out_row, row0, rows, sem):
    slope, facing, shading = targets
    places = (slope, facing.at[0], facing.at[1], shading)
    return [
        pltpu.make_async_copy(
            out.at[n, pl.ds(out_row, rows), :], place.at[pl.ds(row0, rows), :], sem.at[n]
        )
        for n, place in enumerate(places)
    ]


def run(copies):
    for copy in copies:
        copy.start()
    for copy in copies:
        copy.wait()


def write_rows(z, park, q, held, out, sem, targets, row0, lat, total, rows, out_rows, tiles):
    def store(step):
        base = pl.multiple_of(step * SUB, SUB)
        return row_copies(out, targets, base, pl.multiple_of(row0 + base, SUB), SUB, sem)

    stencil(z, park, q, lat * rows + row0, total, out, held, store, out_rows, tiles)
    for copy in row_copies(out, targets, 0, row0, out_rows, sem):
        copy.wait()


def main_kernel(rows, tiles, total, x, lon, near, slope, facing, shading, *scratch):
    z, out, held, sem_x, sem_near, sem_out = scratch[:6]
    lat = lax.axis_index("lat")
    odd = lax.rem(lat, 2)
    own = pl.multiple_of(odd * HALO, HALO)
    beyond = pl.multiple_of((1 - odd) * rows, HALO)
    row0 = pl.multiple_of((1 - odd) * HALO, HALO)
    run(
        column_copies(x, 0, rows, z, own, 0, tiles, sem_x)
        + column_copies(lon, 0, rows, z, own, tiles, 1, sem_x)
        + column_copies(near, 0, HALO, z, beyond, 0, tiles + 1, sem_near)
    )
    write_rows(
        z, scratch[6], scratch[7:], held, out, sem_out, (slope, facing, shading), row0, lat, total, rows,
        rows - HALO, tiles,
    )


def rim_kernel(
    rows, tiles, total, lat_count, x, lon, far, far_lon, _a, _b, _c, slope, facing, shading, *scratch
):
    z, out, held, sem_x, sem_far, sem_out = scratch[:6]
    lat = lax.axis_index("lat")
    odd = lax.rem(lat, 2)
    span = 2 * HALO
    own = pl.multiple_of((1 - odd) * HALO, HALO)
    beyond = pl.multiple_of(odd * span, HALO)
    first = pl.multiple_of(odd * (rows - span), HALO)
    row0 = pl.multiple_of(odd * (rows - HALO), HALO)
    run(
        column_copies(x, first, span, z, own, 0, tiles, sem_x)
        + column_copies(lon, first, span, z, own, tiles, 1, sem_x)
        + column_copies(far, 0, HALO, z, beyond, 0, tiles, sem_far)
        + column_copies(far_lon, 0, HALO, z, beyond, tiles, 1, sem_far)
    )

    @pl.when(lat == 0)
    def _():
        for j in range(tiles + 1):
            z[j, 0:HALO, :] = jnp.broadcast_to(z[j, HALO : HALO + 1, :], (HALO, LANES))

    @pl.when(lat == lat_count - 1)
    def _():
        for j in range(tiles + 1):
            z[j, span:, :] = jnp.broadcast_to(z[j, span - 1 : span, :], (HALO, LANES))

    write_rows(
        z, scratch[6], scratch[7:], held, out, sem_out, (slope, facing, shading), row0, lat, total, rows,
        HALO, tiles,
    )


def scratch_for(out_rows, tiles):
    return [
        pltpu.VMEM((tiles + 1, out_rows + 2 * HALO, LANES), jnp.float32),
        pltpu.VMEM((4, out_rows, tiles * LANES), jnp.float32),
        pltpu.VMEM((2, tiles, SUB, LANES), jnp.float32),
        pltpu.SemaphoreType.DMA((tiles + 1,)),
        pltpu.SemaphoreType.DMA((tiles + 1,)),
        pltpu.SemaphoreType.DMA((4,)),
        pltpu.VMEM((SCALES, tiles + 1, SUB, LANES), jnp.float32),
    ] + [
        pltpu.VMEM((2, tiles, out_rows + 3 * SUB if 2**k < SUB else 2**k, LANES), jnp.float32)
        for k in range(SCALES)
    ]


def cost(out_rows, cols):
    cells = out_rows * cols
    return pl.CostEstimate(flops=200 * cells, bytes_accessed=24 * cells, transcendentals=3 * cells)


def lon_halo(sides):
    count = lax.axis_size("lon")
    if count == 2:
        return lax.ppermute(sides, "lon", [(0, 1), (1, 0)])
    westward = [(i, (i - 1) % count) for i in range(count)]
    eastward = [(i, (i + 1) % count) for i in range(count)]
    east = lax.ppermute(sides[:, :HALO], "lon", westward)
    west = lax.ppermute(sides[:, HALO:], "lon", eastward)
    return jnp.concatenate([east, west], axis=1)


def pairs(first, count):
    ends = [(i, i + 1) for i in range(first, count - 1, 2)]
    return ends + [(b, a) for a, b in ends]


def local(x):
    rows, cols = x.shape
    tiles = cols // LANES
    lat = lax.axis_index("lat")
    count = lax.axis_size("lat")
    odd = lax.rem(lat, 2)
    far_row = odd * (rows - HALO)
    near_row = (1 - odd) * (rows - HALO)

    halo = pl.BlockSpec(memory_space=HALO_SPACE)
    hbm = pl.BlockSpec(memory_space=pltpu.HBM)
    far_block = lax.dynamic_slice(x, (far_row, 0), (HALO, cols))
    near_rows = lax.dynamic_slice(x, (near_row, 0), (HALO, cols))
    held_x, far_block, near_rows = lax.optimization_barrier((x, far_block, near_rows))
    lane = lax.broadcasted_iota(jnp.int32, (rows, LANES), 1)
    sides = jnp.where(lane < HALO, held_x[:, :LANES], held_x[:, cols - LANES :])
    lon = lon_halo(sides)
    far = lax.ppermute(far_block, "lat", pairs(1, count))
    near_block = jnp.concatenate(
        [near_rows, lax.dynamic_slice(lon, (near_row, 0), (HALO, LANES))], axis=1
    )
    near = lax.ppermute(near_block, "lat", pairs(0, count))
    corner_block = lax.dynamic_slice(lon, (far_row, 0), (HALO, LANES))
    far_lon = lax.ppermute(corner_block, "lat", pairs(1, count))

    total = (rows * count, cols * lax.axis_size("lon"))
    shapes = [
        jax.ShapeDtypeStruct((rows, cols), jnp.float32),
        jax.ShapeDtypeStruct((2, rows, cols), jnp.float32),
        jax.ShapeDtypeStruct((rows, cols), jnp.float32),
    ]
    outs = pl.pallas_call(
        functools.partial(main_kernel, rows, tiles, total),
        out_shape=shapes,
        in_specs=[hbm, halo, halo],
        out_specs=[hbm] * 3,
        scratch_shapes=scratch_for(rows - HALO, tiles),
        cost_estimate=cost(rows - HALO, cols),
        compiler_params=pltpu.CompilerParams(vmem_limit_bytes=VMEM_LIMIT),
        name="stencil_main",
    )(x, lon, near)
    return tuple(
        pl.pallas_call(
            functools.partial(rim_kernel, rows, tiles, total, count),
            out_shape=shapes,
            in_specs=[hbm] + [halo] * 3 + [hbm] * 3,
            out_specs=[hbm] * 3,
            input_output_aliases={4: 0, 5: 1, 6: 2},
            scratch_shapes=scratch_for(HALO, tiles),
            cost_estimate=cost(HALO, cols),
            compiler_params=pltpu.CompilerParams(vmem_limit_bytes=VMEM_LIMIT),
            name="stencil_rim",
        )(x, lon, far, far_lon, *outs)
    )


def solution(mesh):
    in_specs = (P("lat", "lon"),)
    out_specs = (P("lat", "lon"), P(None, "lat", "lon"), P("lat", "lon"))

    return jax.shard_map(local, mesh=mesh, in_specs=in_specs, out_specs=out_specs, check_vma=False)
```
